32 devices in a mesh: band: 2 (over x), tm: 16 (over z, y, core).
Axes of the slice: x: 2, y: 2, z: 4, core: 2. Of those that a mesh axis runs over, the one named last changes fastest.
Arguments:
- voltages: bfloat16 [16, 2, 512, 4096], P('band', None, None, 'tm'), parts along dimension 0, may hold values from -12 to 12
- antenna_flags: int32 [32, 16], P('tm', 'band'), parts along dimension 1, may hold values from -2147483648 to 2147483647, as said below
- owned_tile: int32 [16], replicated, may hold values from 0 to 15, each once
Outputs:
- visibility: float32 [512, 16, 2, 512], P('tm', 'band'), parts along dimension 1
The draws below stay inside these ranges and needn't reach their ends.
There are 2 independent parts, one for each index of `band`. The reference program is written for one: setup_inputs(seed, part) draws one part's arguments, and reference() takes and returns one part's arrays. A program takes and returns all parts, laid end to end along the dimension named above; an argument that names none is the same for every part. Nothing has to cross between parts.
Inputs may be any that keep to these rules, and one draw needn't show every extreme that they name: `antenna_flags`: bit b of word w of sub-integration s is 1 where the samples of both polarisations of antenna 32 * w + b are good in that sub-integration of 128 samples, 0 where flagged; all 32 bits of a word are used; some antennas may be flagged in every sub-integration. A permutation: the index k of tm holds the baseline rows of tile owned_tile[k].
All inputs are finite; a program needn't handle non-finite values.
Results may differ from the reference program's by a relative error of at most 0.0003.
Values sent between devices are 32-bit elements; how exact they have to be, the bound alone decides.
A program may use at most 128 MiB of HBM per device.

```python
import math
import jax
import jax.numpy as jnp
from jax import lax

ANTENNAS = 256
INPUTS = 512
FLAG_WORDS = 8
CHANS = 8
SAMPLES_DEV = 256
SUB_LEN = 128
SUBS = 32
TIME = 4096
TILES = 16
N_TM = 16


def gains(key, lowest, highest):
    key_amplitude, key_phase = jax.random.split(key)
    amplitude = jnp.exp(jax.random.uniform(key_amplitude, (INPUTS,), jnp.float32, math.log(lowest), math.log(highest)))
    phase = jax.random.uniform(key_phase, (INPUTS,), jnp.float32, -math.pi, math.pi)
    return (amplitude * jnp.cos(phase), amplitude * jnp.sin(phase))


def source_term(key, lowest, highest):
    key_sky, key_gain = jax.random.split(key)
    sky = jax.random.normal(key_sky, (CHANS, 2, 1, TIME), jnp.float32)
    gain_real, gain_imag = gains(key_gain, lowest, highest)
    gain_real = gain_real[None, :, None]
    gain_imag = gain_imag[None, :, None]
    real_term = gain_real * sky[:, 0] - gain_imag * sky[:, 1]
    imag_term = gain_real * sky[:, 1] + gain_imag * sky[:, 0]
    return jnp.stack([real_term, imag_term], axis=1)


def draw_voltages(key, part):
    key_first = jax.random.fold_in(jax.random.fold_in(key, 11), 0)
    key_noise = jax.random.fold_in(jax.random.fold_in(key, 11), 2)
    noise = jax.random.normal(key_noise, (CHANS, 2, INPUTS, TIME), jnp.float32)
    signal = source_term(key_first, 0.5, 2.0)
    return jnp.clip(signal + noise, -12.0, 12.0).astype(jnp.bfloat16)


def draw_antenna_flags(key, part):
    key_rolled, key_dead = jax.random.split(jax.random.fold_in(key, 23))
    sub_position = jnp.arange(SUBS, dtype=jnp.int32)[:, None]
    threshold = 30 + 60 * sub_position // max(SUBS - 1, 1)
    rolled = jax.random.randint(key_rolled, (SUBS, ANTENNAS), 0, 100)
    ranking = jax.random.permutation(key_dead, ANTENNAS)
    alive = ranking >= max(1, ANTENNAS // 64)
    bits = jnp.where(alive[None, :] & (rolled < threshold), 1, 0).astype(jnp.int32)
    bits = bits.reshape(SUBS, FLAG_WORDS, 32)
    shifts = jnp.arange(32, dtype=jnp.int32)
    return jnp.sum(jnp.left_shift(bits, shifts[None, None, :]), axis=-1, dtype=jnp.int32)


def setup_inputs(seed: int = 0, part: int = 0) -> dict:
    key_list = jax.random.split(jax.random.key(seed), 4)
    own_keys = jax.random.split(jax.random.fold_in(key_list[3], part), 4)
    voltages = draw_voltages(jax.random.fold_in(jax.random.fold_in(key_list[3], part), 71), part)
    antenna_flags = draw_antenna_flags(jax.random.fold_in(jax.random.fold_in(key_list[3], part), 71), part)
    owned_tile = jax.random.permutation(key_list[2], TILES).astype(jnp.int32)
    return {"voltages": voltages, "antenna_flags": antenna_flags, "owned_tile": owned_tile}


def unpack_flags(words):
    shifts = jnp.arange(32, dtype=jnp.int32)
    bits = jnp.bitwise_and(jnp.right_shift(words[:, :, None], shifts[None, None, :]), 1)
    return bits.reshape(words.shape[0], words.shape[1] * 32).astype(jnp.int32)


def reference(voltages, antenna_flags, owned_tile):
    channels = voltages.shape[0]
    inputs = voltages.shape[2]
    block_rows = inputs // N_TM
    good = unpack_flags(antenna_flags)
    input_flags = jnp.repeat(good, 2, axis=1)
    sample_flags = jnp.repeat(input_flags.T, SUB_LEN, axis=1).astype(jnp.bfloat16)
    masked = voltages * sample_flags[None, None]

    def add_block(running, block_index):
        segment = lax.dynamic_slice_in_dim(masked, block_index * SAMPLES_DEV, SAMPLES_DEV, 3).astype(jnp.float32)
        real_part = segment[:, 0]
        imag_part = segment[:, 1]
        right_side = jnp.concatenate([real_part, imag_part], axis=-1)
        left_side = jnp.stack([right_side, jnp.concatenate([imag_part, -real_part], axis=-1)], axis=1)
        return running + jnp.einsum("ckiu,cju->ckij", left_side, right_side), None

    initial = jnp.zeros((channels, 2, inputs, inputs), jnp.float32)
    gram = lax.scan(add_block, initial, jnp.arange(N_TM, dtype=jnp.int32))[0]
    counts = SUB_LEN * jnp.dot(good.T, good)
    row_index = (owned_tile[:, None] * block_rows + jnp.arange(block_rows, dtype=jnp.int32)[None, :]).reshape(-1)
    pair_counts = jnp.repeat(jnp.repeat(counts, 2, axis=0), 2, axis=1)[row_index]
    ordered = jnp.transpose(gram[:, :, row_index, :], (2, 0, 1, 3))
    return ordered / jnp.maximum(pair_counts, 1).astype(jnp.float32)[:, None, None, :]
```

```python
import functools

import jax
import jax.numpy as jnp
from jax import lax
from jax.experimental import pallas as pl
from jax.experimental.pallas import tpu as pltpu
from jax.sharding import PartitionSpec as P

MESH = pl.DeviceIdType.MESH
CORES = 2


def grid_of(mesh):
    count = mesh.shape["tm"]
    ny = 2 if mesh.shape["band"] < 4 and count % (4 * CORES) == 0 else 1
    return count // (ny * CORES), ny


def rank_of(index, nz, ny):
    return ((index % CORES) * ny + (index // CORES) % ny) * nz + index // (CORES * ny)


def kernel(nz, ny, first, owned, flags, volts, summed, mirrored, mask, plane, gram, from_core,
           from_y, from_z, turned, cs, cr, ys, yr, zs, zr, fs, fr):
    count = nz * ny * CORES
    chans, _, tiles, rows, samples = volts.shape
    inputs = tiles * rows
    me = lax.axis_index("tm")
    core = lax.rem(me, CORES)
    y = lax.rem(me // CORES, ny)
    z = me // (CORES * ny)

    def index_at(zz, yy, cc):
        return (zz * ny + yy) * CORES + cc

    barrier = pltpu.get_barrier_semaphore()

    def greet(step, carry):
        pl.semaphore_signal(
            barrier, inc=1, device_id={"tm": lax.rem(me + step, count)}, device_id_type=MESH
        )
        return carry

    lax.fori_loop(1, count, greet, 0)

    subs, words = flags.shape
    length = samples // subs
    span = inputs // words
    shift = lax.broadcasted_iota(jnp.int32, (span, length), 0) // 2
    for word in range(words):
        for sub in range(subs):
            bits = jnp.right_shift(jnp.full((span, length), flags[sub, word], jnp.int32), shift)
            good = jnp.bitwise_and(bits, 1).astype(jnp.float32).astype(mask.dtype)
            good = good.reshape(span // rows, rows, length)
            mask[word * (span // rows) : (word + 1) * (span // rows), :, sub * length : (sub + 1) * length] = good
    pl.semaphore_wait(barrier, count - 1)

    def remote(src, dst, send, recv, target):
        return pltpu.make_async_remote_copy(
            src_ref=src, dst_ref=dst, send_sem=send, recv_sem=recv,
            device_id={"tm": target}, device_id_type=MESH,
        )

    def core_copy(ch):
        return remote(gram.at[ch, 1 - core], from_core.at[ch], cs.at[ch], cr.at[ch], index_at(z, y, 1 - core))

    def y_copy(ch):
        if ny == 1:
            return None
        return remote(gram.at[ch, core, 1 - y], from_y.at[ch], ys.at[ch], yr.at[ch], index_at(z, 1 - y, core))

    def y_last_copy(ch):
        return remote(from_z.at[ch, nz - 2, 1 - y], from_y.at[ch, 0], ys.at[ch], yr.at[ch], index_at(z, 1 - y, core))

    def z_way(ch):
        return 1 - 2 * (ch % 2)

    def z_copy(ch, step, wide):
        way = z_way(ch)
        target = index_at(lax.rem(z + way + nz, nz), y, core)
        dest = lax.rem(z - way * (1 + step) + nz * 2, nz)
        if step == 0:
            src = gram.at[ch, core, :, dest] if wide else gram.at[ch, core, y, dest]
        else:
            src = from_z.at[ch, step - 1] if wide else from_z.at[ch, step - 1, 0]
        dst = from_z.at[ch, step] if wide else from_z.at[ch, step, 0]
        return remote(src, dst, zs.at[ch, step], zr.at[ch, step], target)

    def compute(ch):
        for tile in range(count):
            c, rest = divmod(tile, ny * nz)
            yy, zz = divmod(rest, nz)
            source = owned[index_at(zz, yy, c)]
            good = mask[source]
            for part in range(2):
                value = volts[ch, part, source].astype(mask.dtype) * good
                plane[tile * rows : (tile + 1) * rows, part * samples : (part + 1) * samples] = value
        half = inputs // CORES
        pair = plane[...].astype(jnp.bfloat16)
        for turn in range(CORES):
            c = (core + 1 + turn) % CORES
            part = plane[pl.ds(pl.multiple_of(c * half, half), half), :].astype(jnp.bfloat16)
            other = jnp.concatenate([part[:, samples:], -part[:, :samples]], axis=1)
            dims = (((1,), (1,)), ((), ()))
            total = lax.dot_general(part, pair, dims, preferred_element_type=jnp.float32)
            total += lax.dot_general(other, pair, dims, preferred_element_type=jnp.float32)
            gram[ch, c] = total.reshape(ny, nz, rows, inputs)
            if turn == 0:
                core_copy(ch).start()

    def after_core(ch):
        core_copy(ch).wait()
        gram[ch, core] += from_core[ch]

    def begin(ch):
        after_core(ch)
        if ny == 1:
            z_copy(ch, 0, False).start()
            return

        @pl.when(ch < first)
        def _():
            z_copy(ch, 0, True).start()

        @pl.when(ch >= first)
        def _():
            y_copy(ch).start()

    def body(ch, carry):
        compute(ch)

        @pl.when(ch > 0)
        def _():
            begin(ch - 1)

        return carry

    lax.fori_loop(0, chans, body, 0)
    begin(chans - 1)

    def after_z(ch, step, wide):
        z_copy(ch, step, wide).wait()
        way = z_way(ch)
        dest = lax.rem(z - way * (2 + step) + nz * 2, nz)
        if wide:
            from_z[ch, step] += gram[ch, core, :, dest]
        else:
            value = from_z[ch, step, 0] + gram[ch, core, y, dest]
            if step == nz - 2:
                summed[ch] = value
            else:
                from_z[ch, step, 0] = value
        if step < nz - 2:
            z_copy(ch, step + 1, wide).start()
        elif wide:
            y_last_copy(ch).start()

    def after_y(ch):
        y_copy(ch).wait()
        gram[ch, core, y] += from_y[ch]
        z_copy(ch, 0, False).start()

    def after_last_y(ch):
        y_last_copy(ch).wait()
        summed[ch] = from_z[ch, nz - 2, y] + from_y[ch, 0]

    events = []
    for ch in range(chans):
        if ny == 1:
            for step in range(nz - 1):
                events.append((step * chans + ch, after_z, (ch, step, False)))
        elif ch < first:
            for step in range(nz - 1):
                events.append((8.0 * (step + 1), after_z, (ch, step, True)))
            events.append((8.0 * nz, after_last_y, (ch,)))
        else:
            start = 5.8 * (ch - first + 1)
            events.append((start, after_y, (ch,)))
            for step in range(nz - 1):
                events.append((start + 4.6 * (step + 1), after_z, (ch, step, False)))
    for _, act, args in sorted(events, key=lambda event: event[0]):
        act(*args)

    turned[...] = summed[...].reshape(chans * rows, inputs).T.reshape(count, rows, chans * rows)
    mine = rank_of(me, nz, ny)

    def block_copy(step):
        target = lax.rem(me + step, count)
        return remote(turned.at[rank_of(target, nz, ny)], mirrored.at[mine], fs.at[step], fr.at[step], target)

    def send(step, carry):
        block_copy(step).start()
        return carry

    def finish(step, carry):
        block_copy(step).wait()
        return carry

    lax.fori_loop(1, count, send, 0)
    mirrored[mine] = turned[mine]
    lax.fori_loop(1, count, finish, 0)


def shards(nz, ny, voltages, antenna_flags, owned_tile):
    count = nz * ny * CORES
    me = lax.axis_index("tm")
    chans, _, inputs, samples = voltages.shape
    rows = inputs // count
    sub_length = samples // antenna_flags.shape[0]
    first = chans // 4 if ny > 1 else 0
    held = jnp.bfloat16 if rows % 16 == 0 else jnp.float32
    vmem = pl.BlockSpec(memory_space=pltpu.VMEM)
    smem = pl.BlockSpec(memory_space=pltpu.SMEM)
    dma = pltpu.SemaphoreType.DMA
    summed, mirrored = pl.pallas_call(
        functools.partial(kernel, nz, ny, first),
        out_shape=(
            jax.ShapeDtypeStruct((chans, rows, inputs), jnp.float32),
            jax.ShapeDtypeStruct((count, rows, chans * rows), jnp.float32),
        ),
        in_specs=[smem, smem, vmem],
        out_specs=(vmem, vmem),
        scratch_shapes=[
            pltpu.VMEM((count, rows, samples), held),
            pltpu.VMEM((inputs, 2 * samples), held),
            pltpu.VMEM((chans, CORES, ny, nz, rows, inputs), jnp.float32),
            pltpu.VMEM((chans, ny, nz, rows, inputs), jnp.float32),
            pltpu.VMEM((chans, nz, rows, inputs), jnp.float32),
            pltpu.VMEM((chans, nz - 1, ny, rows, inputs), jnp.float32),
            pltpu.VMEM((count, rows, chans * rows), jnp.float32),
            dma((chans,)), dma((chans,)), dma((chans,)), dma((chans,)),
            dma((chans, nz - 1)), dma((chans, nz - 1)), dma((count,)), dma((count,)),
        ],
        compiler_params=pltpu.CompilerParams(
            collective_id=0, has_side_effects=True, vmem_limit_bytes=60 * 1024 * 1024
        ),
    )(owned_tile, antenna_flags, voltages.reshape(chans, 2, count, rows, samples))

    words = lax.all_gather(antenna_flags, "tm", axis=0, tiled=True)
    shifts = jnp.arange(32, dtype=jnp.int32)
    bits = jnp.bitwise_and(jnp.right_shift(words[:, :, None], shifts), 1)
    good = jnp.broadcast_to(bits[..., None], bits.shape + (2,)).reshape(words.shape[0], count, rows)
    good = good.astype(jnp.bfloat16)
    own = lax.dynamic_index_in_dim(good, owned_tile[me], 1, False)
    counts = jnp.einsum("su,stj->utj", own, good, preferred_element_type=jnp.float32)
    scale = 0.5 / jnp.maximum(sub_length * counts, 1.0)

    holder = jnp.zeros((count,), jnp.int32).at[owned_tile].set(
        rank_of(jnp.arange(count, dtype=jnp.int32), nz, ny)
    )
    direct = summed.reshape(chans, rows, count, rows)[:, :, holder].transpose(1, 0, 2, 3)
    mirror = mirrored.reshape(count, rows, chans, rows)[holder].transpose(1, 2, 0, 3)
    scale = scale[:, None]
    real = ((direct + mirror) * scale).reshape(rows, chans, inputs)
    imag = ((direct - mirror) * scale).reshape(rows, chans, inputs)
    return jnp.stack([real, imag], axis=2)


def solution(mesh):
    nz, ny = grid_of(mesh)
    return jax.shard_map(
        functools.partial(shards, nz, ny),
        mesh=mesh,
        in_specs=(P("band", None, None, "tm"), P("tm", "band"), P()),
        out_specs=P("tm", "band", None, None),
        check_vma=False,
    )
```

```python
import functools

import jax
import jax.numpy as jnp
from jax import lax
from jax.experimental import pallas as pl
from jax.experimental.pallas import tpu as pltpu
from jax.sharding import PartitionSpec as P

MESH = pl.DeviceIdType.MESH
CORES = 2


def grid_of(mesh):
    count = mesh.shape["tm"]
    ny = 2 if mesh.shape["band"] < 4 and count % (4 * CORES) == 0 else 1
    return count // (ny * CORES), ny


def rank_of(index, nz, ny):
    return ((index % CORES) * ny + (index // CORES) % ny) * nz + index // (CORES * ny)


def kernel(nz, ny, first, owned, flags, packed, volts, kept, mirrored, words_all, mask, plane,
           gram, from_core, from_y, from_z, summed, turned, gathered,
           cs, cr, ys, yr, zs, zr, fs, fr, gs, gr):
    count = nz * ny * CORES
    chans, _, tiles, rows, samples = volts.shape
    inputs = tiles * rows
    me = lax.axis_index("tm")
    core = lax.rem(me, CORES)
    y = lax.rem(me // CORES, ny)
    z = me // (CORES * ny)

    def index_at(zz, yy, cc):
        return (zz * ny + yy) * CORES + cc

    barrier = pltpu.get_barrier_semaphore()

    def greet(step, carry):
        pl.semaphore_signal(
            barrier, inc=1, device_id={"tm": lax.rem(me + step, count)}, device_id_type=MESH
        )
        return carry

    lax.fori_loop(1, count, greet, 0)

    subs, words = flags.shape
    length = samples // subs
    span = inputs // words
    shift = lax.broadcasted_iota(jnp.int32, (span, length), 0) // 2
    for word in range(words):
        for sub in range(subs):
            bits = jnp.right_shift(jnp.full((span, length), flags[sub, word], jnp.int32), shift)
            good = jnp.bitwise_and(bits, 1).astype(jnp.float32).astype(mask.dtype)
            good = good.reshape(span // rows, rows, length)
            mask[word * (span // rows) : (word + 1) * (span // rows), :, sub * length : (sub + 1) * length] = good
    pl.semaphore_wait(barrier, count - 1)

    def remote(src, dst, send, recv, target):
        return pltpu.make_async_remote_copy(
            src_ref=src, dst_ref=dst, send_sem=send, recv_sem=recv,
            device_id={"tm": target}, device_id_type=MESH,
        )

    def flag_copy(step):
        target = lax.rem(me + step, count)
        return remote(packed, gathered.at[me], gs.at[step], gr.at[step], target)

    for step in range(1, count):
        flag_copy(step).start()

    def core_copy(ch):
        return remote(gram.at[ch, 1 - core], from_core.at[ch], cs.at[ch], cr.at[ch], index_at(z, y, 1 - core))

    def y_copy(ch):
        if ny == 1:
            return None
        return remote(gram.at[ch, core, 1 - y], from_y.at[ch], ys.at[ch], yr.at[ch], index_at(z, 1 - y, core))

    def y_last_copy(ch):
        return remote(from_z.at[ch, nz - 2, 1 - y], from_y.at[ch, 0], ys.at[ch], yr.at[ch], index_at(z, 1 - y, core))

    def z_way(ch):
        return 1 - 2 * (ch % 2)

    def z_copy(ch, step, wide):
        way = z_way(ch)
        target = index_at(lax.rem(z + way + nz, nz), y, core)
        dest = lax.rem(z - way * (1 + step) + nz * 2, nz)
        if step == 0:
            src = gram.at[ch, core, :, dest] if wide else gram.at[ch, core, y, dest]
        else:
            src = from_z.at[ch, step - 1] if wide else from_z.at[ch, step - 1, 0]
        dst = from_z.at[ch, step] if wide else from_z.at[ch, step, 0]
        return remote(src, dst, zs.at[ch, step], zr.at[ch, step], target)

    def compute(ch):
        for tile in range(count):
            c, rest = divmod(tile, ny * nz)
            yy, zz = divmod(rest, nz)
            source = owned[index_at(zz, yy, c)]
            good = mask[source]
            for part in range(2):
                value = volts[ch, part, source].astype(mask.dtype) * good
                plane[tile * rows : (tile + 1) * rows, part * samples : (part + 1) * samples] = value
        half = inputs // CORES
        pair = plane[...].astype(jnp.bfloat16)
        for turn in range(CORES):
            c = (core + 1 + turn) % CORES
            part = plane[pl.ds(pl.multiple_of(c * half, half), half), :].astype(jnp.bfloat16)
            other = jnp.concatenate([part[:, samples:], -part[:, :samples]], axis=1)
            dims = (((1,), (1,)), ((), ()))
            total = lax.dot_general(part, pair, dims, preferred_element_type=jnp.float32)
            total += lax.dot_general(other, pair, dims, preferred_element_type=jnp.float32)
            gram[ch, c] = total.reshape(ny, nz, rows, inputs)
            if turn == 0:
                core_copy(ch).start()

    def after_core(ch):
        core_copy(ch).wait()
        gram[ch, core] += from_core[ch]

    def begin(ch):
        after_core(ch)
        if ny == 1:
            z_copy(ch, 0, False).start()
            return

        @pl.when(ch < first)
        def _():
            z_copy(ch, 0, True).start()

        @pl.when(ch >= first)
        def _():
            y_copy(ch).start()

    def body(ch, carry):
        compute(ch)

        @pl.when(ch > 0)
        def _():
            begin(ch - 1)

        return carry

    lax.fori_loop(0, chans, body, 0)
    begin(chans - 1)

    for step in range(1, count):
        flag_copy(step).wait()
    for index in range(count):
        value = jnp.where(me == index, packed[...], gathered[index])
        words_all[index * subs : (index + 1) * subs, :] = value[:subs, :words]

    def after_z(ch, step, wide):
        z_copy(ch, step, wide).wait()
        way = z_way(ch)
        dest = lax.rem(z - way * (2 + step) + nz * 2, nz)
        if wide:
            from_z[ch, step] += gram[ch, core, :, dest]
        else:
            value = from_z[ch, step, 0] + gram[ch, core, y, dest]
            if step == nz - 2:
                summed[ch] = value
            else:
                from_z[ch, step, 0] = value
        if step < nz - 2:
            z_copy(ch, step + 1, wide).start()
        elif wide:
            y_last_copy(ch).start()

    def after_y(ch):
        y_copy(ch).wait()
        gram[ch, core, y] += from_y[ch]
        z_copy(ch, 0, False).start()

    def after_last_y(ch):
        y_last_copy(ch).wait()
        summed[ch] = from_z[ch, nz - 2, y] + from_y[ch, 0]

    events = []
    for ch in range(chans):
        if ny == 1:
            for step in range(nz - 1):
                events.append((step * chans + ch, after_z, (ch, step, False)))
        elif ch < first:
            for step in range(nz - 1):
                events.append((8.0 * (step + 1), after_z, (ch, step, True)))
            events.append((8.0 * nz, after_last_y, (ch,)))
        else:
            start = 5.8 * (ch - first + 1)
            events.append((start, after_y, (ch,)))
            for step in range(nz - 1):
                events.append((start + 4.6 * (step + 1), after_z, (ch, step, False)))
    for _, act, args in sorted(events, key=lambda event: event[0]):
        act(*args)

    flipped = summed[...].reshape(chans * rows, inputs).T.reshape(count, rows, chans * rows)
    turned[...] = flipped
    kept[...] = flipped
    mine = rank_of(me, nz, ny)

    def block_copy(step):
        target = lax.rem(me + step, count)
        return remote(turned.at[rank_of(target, nz, ny)], mirrored.at[mine], fs.at[step], fr.at[step], target)

    for step in range(1, count):
        block_copy(step).start()
    for step in range(1, count):
        block_copy(step).wait()
    mirrored[mine] = turned[mine]


def assemble(nz, ny, length, owned, words_all, kept, mirrored, out, pairs, holder):
    count, rows, width = kept.shape
    slots, words = words_all.shape
    inputs = count * rows
    chans = width // rows
    span = inputs // words
    me = lax.axis_index("tm")
    every = words_all[...]
    width = max(span, 128)
    lane = lax.broadcasted_iota(jnp.int32, (slots, width), 1)
    columns = []
    for word in range(0, words, width // span):
        value = jnp.broadcast_to(every[:, word : word + 1], (slots, width))
        for extra in range(1, width // span):
            value = jnp.where(lane >= extra * span, every[:, word + extra : word + extra + 1], value)
        bits = jnp.right_shift(value, (lane % span) // 2)
        columns.append(jnp.bitwise_and(bits, 1).astype(jnp.float32))
    good = jnp.concatenate(columns, axis=1).astype(jnp.bfloat16)
    counts = lax.dot_general(good, good, (((0,), (0,)), ((), ())), preferred_element_type=jnp.float32)
    pairs[...] = counts.reshape(count, rows, inputs)
    for tile in range(count):
        holder[tile] = lax.fori_loop(
            0, count,
            lambda k, found: found + jnp.where(owned[k] == tile, rank_of(k, nz, ny), 0),
            jnp.int32(0),
        )
    scale = 0.5 / jnp.maximum(length * pairs[owned[me]], 1.0)
    direct = jnp.concatenate([kept[holder[tile]] for tile in range(count)], axis=0).T
    each = 128 // rows
    lane = lax.broadcasted_iota(jnp.int32, (rows, 128), 1) // rows
    mirror = [[None] * (count // each) for _ in range(chans)]
    for tile in range(count):
        block = mirrored[holder[tile]]
        if chans * rows < 128:
            block = jnp.concatenate([block, jnp.zeros((rows, 128 - chans * rows), block.dtype)], axis=1)
        place = tile % each
        for ch in range(chans):
            group, offset = divmod(ch * rows, 128)
            piece = block[:, group * 128 : (group + 1) * 128]
            turn = (place * rows - offset) % 128
            if turn:
                piece = pltpu.roll(piece, turn, 1)
            held = mirror[ch][tile // each]
            mirror[ch][tile // each] = piece if held is None else jnp.where(lane == place, piece, held)
    for ch in range(chans):
        left = direct[ch * rows : (ch + 1) * rows]
        right = jnp.concatenate(mirror[ch], axis=1)
        out[:, ch, 0, :] = (left + right) * scale
        out[:, ch, 1, :] = (left - right) * scale


def shards(nz, ny, voltages, antenna_flags, owned_tile):
    count = nz * ny * CORES
    chans, _, inputs, samples = voltages.shape
    rows = inputs // count
    first = chans // 4 if ny > 1 else 0
    held = jnp.bfloat16 if rows % 16 == 0 else jnp.float32
    vmem = pl.BlockSpec(memory_space=pltpu.VMEM)
    smem = pl.BlockSpec(memory_space=pltpu.SMEM)
    dma = pltpu.SemaphoreType.DMA
    sizes = antenna_flags.shape
    padded = jnp.pad(antenna_flags, ((0, -sizes[0] % 8), (0, -sizes[1] % 128)))
    length = samples // sizes[0]
    blocks = jax.ShapeDtypeStruct((count, rows, chans * rows), jnp.float32)
    kept, mirrored, words = pl.pallas_call(
        functools.partial(kernel, nz, ny, first),
        out_shape=(blocks, blocks, jax.ShapeDtypeStruct((count * sizes[0], sizes[1]), jnp.int32)),
        in_specs=[smem, smem, vmem, vmem],
        out_specs=(vmem, vmem, vmem),
        scratch_shapes=[
            pltpu.VMEM((count, rows, samples), held),
            pltpu.VMEM((inputs, 2 * samples), held),
            pltpu.VMEM((chans, CORES, ny, nz, rows, inputs), jnp.float32),
            pltpu.VMEM((chans, ny, nz, rows, inputs), jnp.float32),
            pltpu.VMEM((chans, nz, rows, inputs), jnp.float32),
            pltpu.VMEM((chans, nz - 1, ny, rows, inputs), jnp.float32),
            pltpu.VMEM((chans, rows, inputs), jnp.float32),
            pltpu.VMEM((count, rows, chans * rows), jnp.float32),
            pltpu.VMEM((count,) + padded.shape, jnp.int32),
            dma((chans,)), dma((chans,)), dma((chans,)), dma((chans,)),
            dma((chans, nz - 1)), dma((chans, nz - 1)), dma((count,)), dma((count,)),
            dma((count,)), dma((count,)),
        ],
        compiler_params=pltpu.CompilerParams(
            collective_id=0, has_side_effects=True, vmem_limit_bytes=60 * 1024 * 1024
        ),
    )(owned_tile, antenna_flags, padded, voltages.reshape(chans, 2, count, rows, samples))
    return pl.pallas_call(
        functools.partial(assemble, nz, ny, length),
        out_shape=jax.ShapeDtypeStruct((rows, chans, 2, inputs), jnp.float32),
        in_specs=[smem, vmem, vmem, vmem],
        out_specs=vmem,
        scratch_shapes=[
            pltpu.VMEM((count, rows, inputs), jnp.float32),
            pltpu.SMEM((count,), jnp.int32),
        ],
    )(owned_tile, words, kept, mirrored)


def solution(mesh):
    nz, ny = grid_of(mesh)
    return jax.shard_map(
        functools.partial(shards, nz, ny),
        mesh=mesh,
        in_specs=(P("band", None, None, "tm"), P("tm", "band"), P()),
        out_specs=P("tm", "band", None, None),
        check_vma=False,
    )
```

```python
import functools

import jax
import jax.numpy as jnp
from jax import lax
from jax.experimental import pallas as pl
from jax.experimental.pallas import tpu as pltpu
from jax.sharding import PartitionSpec as P

MESH = pl.DeviceIdType.MESH
CORES = 2


def grid_of(mesh):
    count = mesh.shape["tm"]
    ny = 2 if mesh.shape["band"] < 4 and count % (4 * CORES) == 0 else 1
    return count // (ny * CORES), ny


def rank_of(index, nz, ny):
    return ((index % CORES) * ny + (index // CORES) % ny) * nz + index // (CORES * ny)


def kernel(nz, ny, first, owned, flags, packed, volts, kept, mirrored, words_all, mask, plane,
           gram, from_core, from_y, from_z, summed, turned, gathered,
           cs, cr, ys, yr, zs, zr, fs, fr, gs, gr):
    count = nz * ny * CORES
    chans, _, tiles, rows, samples = volts.shape
    inputs = tiles * rows
    me = lax.axis_index("tm")
    core = lax.rem(me, CORES)
    y = lax.rem(me // CORES, ny)
    z = me // (CORES * ny)

    def index_at(zz, yy, cc):
        return (zz * ny + yy) * CORES + cc

    barrier = pltpu.get_barrier_semaphore()

    def greet(step, carry):
        pl.semaphore_signal(
            barrier, inc=1, device_id={"tm": lax.rem(me + step, count)}, device_id_type=MESH
        )
        return carry

    lax.fori_loop(1, count, greet, 0)

    subs, words = flags.shape
    length = samples // subs
    span = inputs // words
    shift = lax.broadcasted_iota(jnp.int32, (span, length), 0) // 2
    for word in range(words):
        for sub in range(subs):
            bits = jnp.right_shift(jnp.full((span, length), flags[sub, word], jnp.int32), shift)
            good = jnp.bitwise_and(bits, 1).astype(jnp.float32).astype(mask.dtype)
            good = good.reshape(span // rows, rows, length)
            mask[word * (span // rows) : (word + 1) * (span // rows), :, sub * length : (sub + 1) * length] = good
    pl.semaphore_wait(barrier, count - 1)

    def remote(src, dst, send, recv, target):
        return pltpu.make_async_remote_copy(
            src_ref=src, dst_ref=dst, send_sem=send, recv_sem=recv,
            device_id={"tm": target}, device_id_type=MESH,
        )

    def flag_copy(step):
        target = lax.rem(me + step, count)
        return remote(packed, gathered.at[me], gs.at[step], gr.at[step], target)

    for step in range(1, count):
        flag_copy(step).start()

    def core_copy(ch):
        return remote(gram.at[ch, 1 - core], from_core.at[ch], cs.at[ch], cr.at[ch], index_at(z, y, 1 - core))

    def y_copy(ch):
        if ny == 1:
            return None
        return remote(gram.at[ch, core, 1 - y], from_y.at[ch], ys.at[ch], yr.at[ch], index_at(z, 1 - y, core))

    def y_last_copy(ch):
        return remote(from_z.at[ch, nz - 2, 1 - y], from_y.at[ch, 0], ys.at[ch], yr.at[ch], index_at(z, 1 - y, core))

    def z_way(ch):
        return 1 - 2 * (ch % 2)

    def z_copy(ch, step, wide):
        way = z_way(ch)
        target = index_at(lax.rem(z + way + nz, nz), y, core)
        dest = lax.rem(z - way * (1 + step) + nz * 2, nz)
        if step == 0:
            src = gram.at[ch, core, :, dest] if wide else gram.at[ch, core, y, dest]
        else:
            src = from_z.at[ch, step - 1] if wide else from_z.at[ch, step - 1, 0]
        dst = from_z.at[ch, step] if wide else from_z.at[ch, step, 0]
        return remote(src, dst, zs.at[ch, step], zr.at[ch, step], target)

    def compute(ch):
        for tile in range(count):
            c, rest = divmod(tile, ny * nz)
            yy, zz = divmod(rest, nz)
            source = owned[index_at(zz, yy, c)]
            good = mask[source]
            for part in range(2):
                value = volts[ch, part, source].astype(mask.dtype) * good
                plane[tile * rows : (tile + 1) * rows, part * samples : (part + 1) * samples] = value
        half = inputs // CORES
        pair = plane[...].astype(jnp.bfloat16)
        pair = jnp.concatenate([pair, pair], axis=1)
        for turn in range(CORES):
            c = (core + 1 + turn) % CORES
            part = plane[pl.ds(pl.multiple_of(c * half, half), half), :].astype(jnp.bfloat16)
            other = jnp.concatenate([part[:, samples:], -part[:, :samples]], axis=1)
            dims = (((1,), (1,)), ((), ()))
            left = jnp.concatenate([part, other], axis=1)
            total = lax.dot_general(left, pair, dims, preferred_element_type=jnp.float32)
            gram[ch, c] = total.reshape(ny, nz, rows, inputs)
            if turn == 0:
                core_copy(ch).start()

    def after_core(ch):
        core_copy(ch).wait()
        gram[ch, core] += from_core[ch]

    def begin(ch):
        after_core(ch)
        if ny == 1:
            z_copy(ch, 0, False).start()
            return

        wide = jnp.logical_and(ch >= 1, ch < 1 + first)

        @pl.when(wide)
        def _():
            z_copy(ch, 0, True).start()

        @pl.when(jnp.logical_not(wide))
        def _():
            y_copy(ch).start()

    def body(ch, carry):
        compute(ch)

        @pl.when(ch > 0)
        def _():
            begin(ch - 1)

        return carry

    lax.fori_loop(0, chans, body, 0)
    begin(chans - 1)

    for step in range(1, count):
        flag_copy(step).wait()
    for index in range(count):
        value = jnp.where(me == index, packed[...], gathered[index])
        words_all[index * subs : (index + 1) * subs, :] = value[:subs, :words]

    def after_z(ch, step, wide):
        z_copy(ch, step, wide).wait()
        way = z_way(ch)
        dest = lax.rem(z - way * (2 + step) + nz * 2, nz)
        if wide:
            from_z[ch, step] += gram[ch, core, :, dest]
        else:
            value = from_z[ch, step, 0] + gram[ch, core, y, dest]
            if step == nz - 2:
                summed[ch] = value
            else:
                from_z[ch, step, 0] = value
        if step < nz - 2:
            z_copy(ch, step + 1, wide).start()
        elif wide:
            y_last_copy(ch).start()

    def after_y(ch):
        y_copy(ch).wait()
        gram[ch, core, y] += from_y[ch]
        z_copy(ch, 0, False).start()

    def after_last_y(ch):
        y_last_copy(ch).wait()
        summed[ch] = from_z[ch, nz - 2, y] + from_y[ch, 0]

    groups = turned.shape[0]
    size = chans // groups
    mine = rank_of(me, nz, ny)

    def block_copy(group, step):
        target = lax.rem(me + step, count)
        return remote(
            turned.at[group, rank_of(target, nz, ny)], mirrored.at[group, mine],
            fs.at[group, step], fr.at[group, step], target,
        )

    def exchange(group):
        value = summed[group * size : (group + 1) * size].reshape(size * rows, inputs)
        value = value.T.reshape(count, rows, size * rows)
        turned[group] = value
        kept[group] = value
        for step in range(1, count):
            block_copy(group, step).start()

    events = []
    ends = [0.0] * groups
    start = 0.0
    for ch in range(chans):
        mark = len(events)
        if ny == 1:
            for step in range(nz - 1):
                events.append((step * chans + ch, after_z, (ch, step, False)))
        elif 1 <= ch < 1 + first:
            for step in range(nz - 1):
                events.append((8.0 * (step + 1), after_z, (ch, step, True)))
            events.append((8.0 * nz, after_last_y, (ch,)))
        else:
            start += 5.8
            events.append((start, after_y, (ch,)))
            for step in range(nz - 1):
                events.append((start + 4.6 * (step + 1), after_z, (ch, step, False)))
        last = max(event[0] for event in events[mark:])
        ends[ch // size] = max(ends[ch // size], last + 0.01)
    for group in range(groups):
        events.append((ends[group], exchange, (group,)))
    for _, act, args in sorted(events, key=lambda event: event[0]):
        act(*args)
    for group in range(groups):
        for step in range(1, count):
            block_copy(group, step).wait()
        mirrored[group, mine] = turned[group, mine]


def assemble(nz, ny, length, owned, words_all, kept, mirrored, out, pairs, holder):
    groups, count, rows, width = kept.shape
    slots, words = words_all.shape
    inputs = count * rows
    chans = groups * width // rows
    size = chans // groups
    span = inputs // words
    me = lax.axis_index("tm")
    every = words_all[...]
    width = max(span, 128)
    lane = lax.broadcasted_iota(jnp.int32, (slots, width), 1)
    columns = []
    for word in range(0, words, width // span):
        value = jnp.broadcast_to(every[:, word : word + 1], (slots, width))
        for extra in range(1, width // span):
            value = jnp.where(lane >= extra * span, every[:, word + extra : word + extra + 1], value)
        bits = jnp.right_shift(value, (lane % span) // 2)
        columns.append(jnp.bitwise_and(bits, 1).astype(jnp.float32))
    good = jnp.concatenate(columns, axis=1).astype(jnp.bfloat16)
    counts = lax.dot_general(good, good, (((0,), (0,)), ((), ())), preferred_element_type=jnp.float32)
    pairs[...] = counts.reshape(count, rows, inputs)
    for tile in range(count):
        holder[tile] = lax.fori_loop(
            0, count,
            lambda k, found: found + jnp.where(owned[k] == tile, rank_of(k, nz, ny), 0),
            jnp.int32(0),
        )
    scale = 0.5 / jnp.maximum(length * pairs[owned[me]], 1.0)
    each = 128 // rows
    lane = lax.broadcasted_iota(jnp.int32, (rows, 128), 1) // rows
    for group in range(groups):
        direct = jnp.concatenate([kept[group, holder[tile]] for tile in range(count)], axis=0).T
        mirror = [[None] * (count // each) for _ in range(size)]
        for tile in range(count):
            piece = mirrored[group, holder[tile]]
            if size * rows < 128:
                piece = jnp.concatenate([piece, jnp.zeros((rows, 128 - size * rows), piece.dtype)], axis=1)
            place = tile % each
            for ch in range(size):
                turn = (place - ch) * rows % 128
                moved = pltpu.roll(piece, turn, 1) if turn else piece
                held = mirror[ch][tile // each]
                mirror[ch][tile // each] = moved if held is None else jnp.where(lane == place, moved, held)
        for ch in range(size):
            left = direct[ch * rows : (ch + 1) * rows]
            right = jnp.concatenate(mirror[ch], axis=1)
            out[:, group * size + ch, 0, :] = (left + right) * scale
            out[:, group * size + ch, 1, :] = (left - right) * scale


def shards(nz, ny, voltages, antenna_flags, owned_tile):
    count = nz * ny * CORES
    chans, _, inputs, samples = voltages.shape
    rows = inputs // count
    first = chans // 4 if ny > 1 else 0
    held = jnp.bfloat16 if rows % 16 == 0 else jnp.float32
    vmem = pl.BlockSpec(memory_space=pltpu.VMEM)
    smem = pl.BlockSpec(memory_space=pltpu.SMEM)
    dma = pltpu.SemaphoreType.DMA
    sizes = antenna_flags.shape
    padded = jnp.pad(antenna_flags, ((0, -sizes[0] % 8), (0, -sizes[1] % 128)))
    length = samples // sizes[0]
    groups = max(1, chans * rows // 128)
    shape = (groups, count, rows, chans // groups * rows)
    blocks = jax.ShapeDtypeStruct(shape, jnp.float32)
    kept, mirrored, words = pl.pallas_call(
        functools.partial(kernel, nz, ny, first),
        out_shape=(blocks, blocks, jax.ShapeDtypeStruct((count * sizes[0], sizes[1]), jnp.int32)),
        in_specs=[smem, smem, vmem, vmem],
        out_specs=(vmem, vmem, vmem),
        scratch_shapes=[
            pltpu.VMEM((count, rows, samples), held),
            pltpu.VMEM((inputs, 2 * samples), held),
            pltpu.VMEM((chans, CORES, ny, nz, rows, inputs), jnp.float32),
            pltpu.VMEM((chans, ny, nz, rows, inputs), jnp.float32),
            pltpu.VMEM((chans, nz, rows, inputs), jnp.float32),
            pltpu.VMEM((chans, nz - 1, ny, rows, inputs), jnp.float32),
            pltpu.VMEM((chans, rows, inputs), jnp.float32),
            pltpu.VMEM(shape, jnp.float32),
            pltpu.VMEM((count,) + padded.shape, jnp.int32),
            dma((chans,)), dma((chans,)), dma((chans,)), dma((chans,)),
            dma((chans, nz - 1)), dma((chans, nz - 1)), dma((groups, count)), dma((groups, count)),
            dma((count,)), dma((count,)),
        ],
        compiler_params=pltpu.CompilerParams(
            collective_id=0, has_side_effects=True, vmem_limit_bytes=60 * 1024 * 1024
        ),
    )(owned_tile, antenna_flags, padded, voltages.reshape(chans, 2, count, rows, samples))
    return pl.pallas_call(
        functools.partial(assemble, nz, ny, length),
        out_shape=jax.ShapeDtypeStruct((rows, chans, 2, inputs), jnp.float32),
        in_specs=[smem, vmem, vmem, vmem],
        out_specs=vmem,
        scratch_shapes=[
            pltpu.VMEM((count, rows, inputs), jnp.float32),
            pltpu.SMEM((count,), jnp.int32),
        ],
    )(owned_tile, words, kept, mirrored)


def solution(mesh):
    nz, ny = grid_of(mesh)
    return jax.shard_map(
        functools.partial(shards, nz, ny),
        mesh=mesh,
        in_specs=(P("band", None, None, "tm"), P("tm", "band"), P()),
        out_specs=P("tm", "band", None, None),
        check_vma=False,
    )
```

```python
import functools

import jax
import jax.numpy as jnp
from jax import lax
from jax.experimental import pallas as pl
from jax.experimental.pallas import tpu as pltpu
from jax.sharding import PartitionSpec as P

MESH = pl.DeviceIdType.MESH
CORES = 2


def grid_of(mesh):
    count = mesh.shape["tm"]
    ny = 2 if mesh.shape["band"] < 4 and count % (4 * CORES) == 0 else 1
    return count // (ny * CORES), ny


def rank_of(index, nz, ny):
    return ((index % CORES) * ny + (index // CORES) % ny) * nz + index // (CORES * ny)


def kernel(nz, ny, first, owned, flags, packed, volts, kept, mirrored, words_all, mask, plane,
           gram, from_core, from_y, from_z, summed, turned, gathered,
           cs, cr, ys, yr, zs, zr, fs, fr, gs, gr):
    count = nz * ny * CORES
    chans, _, tiles, rows, samples = volts.shape
    inputs = tiles * rows
    me = lax.axis_index("tm")
    core = lax.rem(me, CORES)
    y = lax.rem(me // CORES, ny)
    z = me // (CORES * ny)

    def index_at(zz, yy, cc):
        return (zz * ny + yy) * CORES + cc

    barrier = pltpu.get_barrier_semaphore()

    def greet(step, carry):
        pl.semaphore_signal(
            barrier, inc=1, device_id={"tm": lax.rem(me + step, count)}, device_id_type=MESH
        )
        return carry

    lax.fori_loop(1, count, greet, 0)

    subs, words = flags.shape
    length = samples // subs
    span = inputs // words
    shift = lax.broadcasted_iota(jnp.int32, (span, length), 0) // 2
    for word in range(words):
        for sub in range(subs):
            bits = jnp.right_shift(jnp.full((span, length), flags[sub, word], jnp.int32), shift)
            good = jnp.bitwise_and(bits, 1).astype(jnp.float32).astype(mask.dtype)
            good = good.reshape(span // rows, rows, length)
            mask[word * (span // rows) : (word + 1) * (span // rows), :, sub * length : (sub + 1) * length] = good
    pl.semaphore_wait(barrier, count - 1)

    def remote(src, dst, send, recv, target):
        return pltpu.make_async_remote_copy(
            src_ref=src, dst_ref=dst, send_sem=send, recv_sem=recv,
            device_id={"tm": target}, device_id_type=MESH,
        )

    def flag_copy(step):
        target = lax.rem(me + step, count)
        return remote(packed, gathered.at[me], gs.at[step], gr.at[step], target)

    for step in range(1, count):
        flag_copy(step).start()

    def core_copy(ch):
        return remote(gram.at[ch, 1 - core], from_core.at[ch], cs.at[ch], cr.at[ch], index_at(z, y, 1 - core))

    def y_copy(ch):
        if ny == 1:
            return None
        return remote(gram.at[ch, core, 1 - y], from_y.at[ch], ys.at[ch], yr.at[ch], index_at(z, 1 - y, core))

    def y_last_copy(ch):
        return remote(from_z.at[ch, nz - 2, 1 - y], from_y.at[ch, 0], ys.at[ch], yr.at[ch], index_at(z, 1 - y, core))

    def z_way(ch):
        return 1 - 2 * (ch % 2)

    def z_copy(ch, step, wide):
        way = z_way(ch)
        target = index_at(lax.rem(z + way + nz, nz), y, core)
        dest = lax.rem(z - way * (1 + step) + nz * 2, nz)
        if step == 0:
            src = gram.at[ch, core, :, dest] if wide else gram.at[ch, core, y, dest]
        else:
            src = from_z.at[ch, step - 1] if wide else from_z.at[ch, step - 1, 0]
        dst = from_z.at[ch, step] if wide else from_z.at[ch, step, 0]
        return remote(src, dst, zs.at[ch, step], zr.at[ch, step], target)

    def compute(ch):
        for tile in range(count):
            c, rest = divmod(tile, ny * nz)
            yy, zz = divmod(rest, nz)
            source = owned[index_at(zz, yy, c)]
            good = mask[source]
            for part in range(2):
                value = volts[ch, part, source].astype(mask.dtype) * good
                plane[tile * rows : (tile + 1) * rows, part * samples : (part + 1) * samples] = value
        half = inputs // CORES
        pair = plane[...].astype(jnp.bfloat16)
        pair = jnp.concatenate([pair, pair], axis=1)
        for turn in range(CORES):
            c = (core + 1 + turn) % CORES
            part = plane[pl.ds(pl.multiple_of(c * half, half), half), :].astype(jnp.bfloat16)
            other = jnp.concatenate([part[:, samples:], -part[:, :samples]], axis=1)
            dims = (((1,), (1,)), ((), ()))
            left = jnp.concatenate([part, other], axis=1)
            total = lax.dot_general(left, pair, dims, preferred_element_type=jnp.float32)
            gram[ch, c] = total.reshape(ny, nz, rows, inputs)
            if turn == 0:
                core_copy(ch).start()

    def after_core(ch):
        core_copy(ch).wait()
        gram[ch, core] += from_core[ch]

    def begin(ch):
        after_core(ch)
        if ny == 1:
            z_copy(ch, 0, False).start()
            return

        wide = jnp.logical_and(ch >= 1, ch < 1 + first)

        @pl.when(wide)
        def _():
            z_copy(ch, 0, True).start()

        @pl.when(jnp.logical_not(wide))
        def _():
            y_copy(ch).start()

    def body(ch, carry):
        compute(ch)

        @pl.when(ch > 0)
        def _():
            begin(ch - 1)

        return carry

    lax.fori_loop(0, chans, body, 0)
    begin(chans - 1)

    for step in range(1, count):
        flag_copy(step).wait()
    for index in range(count):
        value = jnp.where(me == index, packed[...], gathered[index])
        words_all[index * subs : (index + 1) * subs, :] = value[:subs, :words]

    def after_z(ch, step, wide):
        z_copy(ch, step, wide).wait()
        way = z_way(ch)
        dest = lax.rem(z - way * (2 + step) + nz * 2, nz)
        if wide:
            from_z[ch, step] += gram[ch, core, :, dest]
        else:
            value = from_z[ch, step, 0] + gram[ch, core, y, dest]
            if step == nz - 2:
                summed[ch] = value
            else:
                from_z[ch, step, 0] = value
        if step < nz - 2:
            z_copy(ch, step + 1, wide).start()
        elif wide:
            y_last_copy(ch).start()

    def after_y(ch):
        y_copy(ch).wait()
        gram[ch, core, y] += from_y[ch]
        z_copy(ch, 0, False).start()

    def after_last_y(ch):
        y_last_copy(ch).wait()
        summed[ch] = from_z[ch, nz - 2, y] + from_y[ch, 0]

    groups = turned.shape[0]
    size = chans // groups
    mine = rank_of(me, nz, ny)

    def block_copy(group, step):
        target = lax.rem(me + step, count)
        return remote(
            turned.at[group, rank_of(target, nz, ny)], mirrored.at[group, mine],
            fs.at[group, step], fr.at[group, step], target,
        )

    def exchange(group):
        value = summed[group * size : (group + 1) * size].reshape(size * rows, inputs)
        value = value.T.reshape(count, rows, size * rows)
        turned[group] = value
        kept[group] = value
        for step in range(1, count):
            block_copy(group, step).start()

    events = []
    ends = [0.0] * groups
    start = 0.0
    for ch in range(chans):
        mark = len(events)
        if ny == 1:
            for step in range(nz - 1):
                events.append((step * chans + ch, after_z, (ch, step, False)))
        elif 1 <= ch < 1 + first:
            for step in range(nz - 1):
                events.append((8.0 * (step + 1), after_z, (ch, step, True)))
            events.append((8.0 * nz, after_last_y, (ch,)))
        else:
            start += 5.8
            events.append((start, after_y, (ch,)))
            for step in range(nz - 1):
                events.append((start + 3.8 * (step + 1), after_z, (ch, step, False)))
        last = max(event[0] for event in events[mark:])
        ends[ch // size] = max(ends[ch // size], last + 0.01)
    for group in range(groups):
        events.append((ends[group], exchange, (group,)))
    for _, act, args in sorted(events, key=lambda event: event[0]):
        act(*args)
    for group in range(groups):
        for step in range(1, count):
            block_copy(group, step).wait()
        mirrored[group, mine] = turned[group, mine]


def assemble(nz, ny, length, owned, words_all, kept, mirrored, out, pairs, holder):
    groups, count, rows, width = kept.shape
    slots, words = words_all.shape
    inputs = count * rows
    chans = groups * width // rows
    size = chans // groups
    span = inputs // words
    me = lax.axis_index("tm")
    every = words_all[...]
    width = max(span, 128)
    lane = lax.broadcasted_iota(jnp.int32, (slots, width), 1)
    columns = []
    for word in range(0, words, width // span):
        value = jnp.broadcast_to(every[:, word : word + 1], (slots, width))
        for extra in range(1, width // span):
            value = jnp.where(lane >= extra * span, every[:, word + extra : word + extra + 1], value)
        bits = jnp.right_shift(value, (lane % span) // 2)
        columns.append(jnp.bitwise_and(bits, 1).astype(jnp.float32))
    good = jnp.concatenate(columns, axis=1).astype(jnp.bfloat16)
    counts = lax.dot_general(good, good, (((0,), (0,)), ((), ())), preferred_element_type=jnp.float32)
    pairs[...] = counts.reshape(count, rows, inputs)
    for tile in range(count):
        holder[tile] = lax.fori_loop(
            0, count,
            lambda k, found: found + jnp.where(owned[k] == tile, rank_of(k, nz, ny), 0),
            jnp.int32(0),
        )
    scale = 0.5 / jnp.maximum(length * pairs[owned[me]], 1.0)
    each = 128 // rows
    lane = lax.broadcasted_iota(jnp.int32, (rows, 128), 1) // rows
    for group in range(groups):
        direct = jnp.concatenate([kept[group, holder[tile]] for tile in range(count)], axis=0).T
        mirror = [[None] * (count // each) for _ in range(size)]
        for tile in range(count):
            piece = mirrored[group, holder[tile]]
            if size * rows < 128:
                piece = jnp.concatenate([piece, jnp.zeros((rows, 128 - size * rows), piece.dtype)], axis=1)
            place = tile % each
            for ch in range(size):
                turn = (place - ch) * rows % 128
                moved = pltpu.roll(piece, turn, 1) if turn else piece
                held = mirror[ch][tile // each]
                mirror[ch][tile // each] = moved if held is None else jnp.where(lane == place, moved, held)
        for ch in range(size):
            left = direct[ch * rows : (ch + 1) * rows]
            right = jnp.concatenate(mirror[ch], axis=1)
            out[:, group * size + ch, 0, :] = (left + right) * scale
            out[:, group * size + ch, 1, :] = (left - right) * scale


def shards(nz, ny, voltages, antenna_flags, owned_tile):
    count = nz * ny * CORES
    chans, _, inputs, samples = voltages.shape
    rows = inputs // count
    first = chans // 4 if ny > 1 else 0
    held = jnp.bfloat16 if rows % 16 == 0 else jnp.float32
    vmem = pl.BlockSpec(memory_space=pltpu.VMEM)
    smem = pl.BlockSpec(memory_space=pltpu.SMEM)
    dma = pltpu.SemaphoreType.DMA
    sizes = antenna_flags.shape
    length = samples // sizes[0]
    groups = max(1, chans * rows // 128)
    shape = (groups, count, rows, chans // groups * rows)
    blocks = jax.ShapeDtypeStruct(shape, jnp.float32)
    kept, mirrored, words = pl.pallas_call(
        functools.partial(kernel, nz, ny, first),
        out_shape=(blocks, blocks, jax.ShapeDtypeStruct((count * sizes[0], sizes[1]), jnp.int32)),
        in_specs=[smem, smem, vmem, vmem],
        out_specs=(vmem, vmem, vmem),
        scratch_shapes=[
            pltpu.VMEM((count, rows, samples), held),
            pltpu.VMEM((inputs, 2 * samples), held),
            pltpu.VMEM((chans, CORES, ny, nz, rows, inputs), jnp.float32),
            pltpu.VMEM((chans, ny, nz, rows, inputs), jnp.float32),
            pltpu.VMEM((chans, nz, rows, inputs), jnp.float32),
            pltpu.VMEM((chans, nz - 1, ny, rows, inputs), jnp.float32),
            pltpu.VMEM((chans, rows, inputs), jnp.float32),
            pltpu.VMEM(shape, jnp.float32),
            pltpu.VMEM((count,) + sizes, jnp.int32),
            dma((chans,)), dma((chans,)), dma((chans,)), dma((chans,)),
            dma((chans, nz - 1)), dma((chans, nz - 1)), dma((groups, count)), dma((groups, count)),
            dma((count,)), dma((count,)),
        ],
        compiler_params=pltpu.CompilerParams(
            collective_id=0, has_side_effects=True, vmem_limit_bytes=60 * 1024 * 1024
        ),
    )(owned_tile, antenna_flags, antenna_flags, voltages.reshape(chans, 2, count, rows, samples))
    return pl.pallas_call(
        functools.partial(assemble, nz, ny, length),
        out_shape=jax.ShapeDtypeStruct((rows, chans, 2, inputs), jnp.float32),
        in_specs=[smem, vmem, vmem, vmem],
        out_specs=vmem,
        scratch_shapes=[
            pltpu.VMEM((count, rows, inputs), jnp.float32),
            pltpu.SMEM((count,), jnp.int32),
        ],
    )(owned_tile, words, kept, mirrored)


def solution(mesh):
    nz, ny = grid_of(mesh)
    return jax.shard_map(
        functools.partial(shards, nz, ny),
        mesh=mesh,
        in_specs=(P("band", None, None, "tm"), P("tm", "band"), P()),
        out_specs=P("tm", "band", None, None),
        check_vma=False,
    )
```
